128 devices in a mesh: grp: 4 (over z), dev: 32 (over x, y, core).
Axes of the slice: x: 4, y: 4, z: 4, core: 2. Of those that a mesh axis runs over, the one named last changes fastest.
Arguments:
- qkv_weight: bfloat16 [2, 4608, 8192], P(None, ('grp', 'dev')), may hold values from -0.09375 to 0.09375
- gate_up_weight: bfloat16 [2, 4608, 73728], P(None, ('grp', 'dev')), may hold values from -0.09375 to 0.09375
- head_slot: int32 [64], replicated, may hold values from 0 to 63, each once
- layer_ids: int32 [2], replicated, may hold values from 0 to 45
- stored_qkv: int32 [46, 64], replicated, may hold values from -16384 to 16383
- stored_gate_up: int32 [46, 576], replicated, may hold values from -16384 to 16383
Outputs:
- served_qkv: bfloat16 [2, 4608, 8192], P(None, 'grp', 'dev')
- served_gate_up: bfloat16 [2, 4608, 73728], P(None, 'grp', 'dev')
- qkv_mismatch: float32 [2, 64], P(None, 'dev')
- gate_up_mismatch: float32 [2, 576], P(None, 'dev')
The draws below stay inside these ranges and needn't reach their ends.
Inputs may be any that keep to these rules, and one draw needn't show every extreme that they name: `head_slot`: each of the 64 heads appears once.
All inputs are finite; a program needn't handle non-finite values.
Results may differ from the reference program's by a relative error of at most 0.0004.
Values may be sent and summed in bfloat16 or wider, within the bound.
No kernel may reach another device: no remote copies, remote signals or barrier semaphores. Data moves between devices by JAX's collectives and lax.ppermute only.
A program may use at most 128 MiB of HBM per device.

```python
import jax
import jax.numpy as jnp
from jax import lax

D = 4608
HEAD_DIM = 128
FF = 36864
STORED = 46
LAYERS = 2
BLK = 128
NHEAD = 64
N_DEV = 32


def touch_ends(values, key, low, largest):
    place = [jax.random.randint(jax.random.fold_in(key, axis), (), 0, length) for axis, length in enumerate(values.shape)]
    longest = values.shape.index(max(values.shape))
    next_to = place[:longest] + [(place[longest] + 1) % values.shape[longest]] + place[longest + 1:]
    return values.at[tuple(place)].set(low).at[tuple(next_to)].set(largest)


def steps_of(rng, shape, split, smallest, high):
    factor_of, own = 1.0, jax.random.fold_in(rng, 6)
    for axis_at, shards_of in split:
        draws = jnp.exp(jax.random.uniform(jax.random.fold_in(own, axis_at), (shards_of,), jnp.float32, smallest / len(split), high / len(split)))
        factor_of = factor_of * jnp.repeat(draws, shape[axis_at] // shards_of).reshape([-1 if axis == axis_at else 1 for axis in range(len(shape))])
    return factor_of


def centred(key, dims, spread, bound, split=(), dtype=jnp.bfloat16):
    factor_of = steps_of(key, dims, split, -0.22, 0.18) if split else 1.0
    values = jax.random.normal(key, dims, jnp.float32) * spread * factor_of
    return jnp.minimum(jnp.maximum(values, -bound), bound).astype(dtype)


def setup_inputs(seed: int = 0) -> dict:
    key_of = jax.random.split(jax.random.key(seed), 7)
    return {
        "qkv_weight": centred(key_of[0], (LAYERS, D, NHEAD * HEAD_DIM), D ** -0.5, 0.09375, ((1, 128),)),
        "gate_up_weight": centred(key_of[1], (LAYERS, D, 2 * FF), D ** -0.5, 0.09375, ((1, 128),)),
        "head_slot": jax.random.permutation(key_of[2], NHEAD).astype(jnp.int32),
        "layer_ids": jax.random.randint(key_of[3], (LAYERS,), 0, STORED).astype(jnp.int32),
        "stored_qkv": touch_ends(jax.random.randint(key_of[4], (STORED, NHEAD), -16384, 16384), jax.random.fold_in(key_of[4], 1), -16384, 16383).astype(jnp.int32),
        "stored_gate_up": touch_ends(jax.random.randint(key_of[5], (STORED, 2 * FF // BLK), -16384, 16384), jax.random.fold_in(key_of[5], 1), -16384, 16383).astype(jnp.int32),
    }


stored_unit = 1.0 / 1024.0


def reference(qkv_weight, gate_up_weight, head_slot, layer_ids, stored_qkv, stored_gate_up):
    width = FF // N_DEV
    served_qkv = qkv_weight.reshape(LAYERS, D, NHEAD, HEAD_DIM)[:, :, head_slot, :].reshape(LAYERS, D, NHEAD * HEAD_DIM)
    served_gate_up = gate_up_weight.reshape(LAYERS, D, 2, N_DEV, width).transpose(0, 1, 3, 2, 4).reshape(LAYERS, D, 2 * FF)

    def layer_sums(pair):
        qkv_layer, gate_layer = pair
        head_sum = jnp.sum(qkv_layer.astype(jnp.float32).reshape(D, NHEAD, HEAD_DIM), axis=(0, 2))
        block_sum = jnp.sum(gate_layer.astype(jnp.float32).reshape(D, 2 * FF // BLK, BLK), axis=(0, 2))
        return head_sum, block_sum

    head_sum, block_sum = lax.map(layer_sums, (served_qkv, served_gate_up))
    picked_qkv = stored_qkv[layer_ids][:, head_slot].astype(jnp.float32)
    picked_gate = stored_gate_up[layer_ids].reshape(LAYERS, 2, N_DEV, width // BLK)
    picked_gate = picked_gate.transpose(0, 2, 1, 3).reshape(LAYERS, 2 * FF // BLK).astype(jnp.float32)
    qkv_mismatch = head_sum - picked_qkv * stored_unit
    gate_up_mismatch = block_sum - picked_gate * stored_unit
    return served_qkv, served_gate_up, qkv_mismatch, gate_up_mismatch
```

```python
import functools

import jax
import jax.numpy as jnp
import numpy as np
from jax import lax
from jax.experimental import pallas as pl
from jax.experimental.pallas import tpu as pltpu
from jax.sharding import PartitionSpec as P


HEAD_DIM = 128
FF = 36864
STORED = 46
BLK = 128
NHEAD = 64

stored_unit = 1.0 / 1024.0

ORDER = [(1, 0), (3, 0), (0, 1), (0, 3), (1, 1), (3, 3), (1, 3), (3, 1), (2, 0), (0, 2), (2, 1), (2, 3), (1, 2), (3, 2), (2, 2)]

MOVES = [(dx, dy, dc) for dx, dy in ORDER for dc in (0, 1)] + [(0, 0, 1), (0, 0, 0)]
COUNTS = [2, 4, 6, 8, 12]

ROWS = 36
TILES = FF // 32 // 128
PIECE = (2 * ROWS + 8, TILES, 2, 128)
GATE_ROWS = ROWS * TILES * 2
HEAD_ROWS = ROWS * 2


def place_of(me):
    return me // 8, (me // 2) % 4, me % 2


def moved_pairs(dx, dy, dc):
    pairs = []
    for me in range(32):
        x, y, c = place_of(me)
        pairs.append((me, (((x + dx) % 4) * 4 + (y + dy) % 4) * 2 + (c ^ dc)))
    return pairs


def in_hbm(x):
    return pltpu.with_memory_space_constraint(x, pltpu.HBM)


def in_vmem(x):
    return pltpu.with_memory_space_constraint(x, pltpu.VMEM)


def here():
    me = lax.axis_index("dev")
    return lax.div(me, 8), lax.rem(lax.div(me, 2), 4), lax.rem(me, 2)


def cut_kernel(shifts, heads, gate, qkv, *rest):
    outs, (held, in_sems, out_sems) = rest[-3 - len(shifts) : -3], rest[-3:]
    x, y, c = here()
    loads = []
    for i, (dx, dy, dc) in enumerate(shifts):
        owner = (lax.rem(x + dx, 4) * 4 + lax.rem(y + dy, 4)) * 2 + lax.rem(c + dc, 2)
        loads.append(
            [
                pltpu.make_async_copy(
                    gate.at[:, pl.ds(p * 32 * TILES + owner * TILES, TILES)],
                    held.at[i, pl.ds(p * ROWS, ROWS)],
                    in_sems.at[i, p],
                )
                for p in range(2)
            ]
            + [
                pltpu.make_async_copy(
                    qkv.at[:, :, heads[2 * owner + k]],
                    held.at[i, pl.ds(2 * ROWS + 4 * k, 4)],
                    in_sems.at[i, 2 + k],
                )
                for k in range(2)
            ]
        )
    stores = [pltpu.make_async_copy(held.at[i], out, out_sems.at[i]) for i, out in enumerate(outs)]
    for load in loads:
        for copy in load:
            copy.start()
    for load, store in zip(loads, stores):
        for copy in load:
            copy.wait()
        store.start()
    for store in stores:
        store.wait()


def cut(shifts, heads, gate, qkv, after):
    size = int(np.prod(PIECE)) * 2 * len(shifts)
    return pl.pallas_call(
        functools.partial(cut_kernel, shifts),
        out_shape=[pltpu.HBM(PIECE, jnp.bfloat16)] * len(shifts),
        in_specs=[pl.BlockSpec(memory_space=pltpu.SMEM)] + [pl.BlockSpec(memory_space=pl.ANY)] * (2 + len(after)),
        out_specs=[pl.BlockSpec(memory_space=pl.ANY)] * len(shifts),
        scratch_shapes=[
            pltpu.VMEM((len(shifts), *PIECE), jnp.bfloat16),
            pltpu.SemaphoreType.DMA((len(shifts), 4)),
            pltpu.SemaphoreType.DMA((len(shifts),)),
        ],
        compiler_params=pltpu.CompilerParams(vmem_limit_bytes=(len(shifts) + 1) << 19),
        cost_estimate=pl.CostEstimate(flops=size, bytes_accessed=2 * size, transcendentals=0),
        name="cut",
    )(heads, gate, qkv, *after)


def turns():
    gate = np.zeros((168, 144), np.float32)
    for r in range(8):
        for j in range(TILES):
            for l in range(2):
                k = (r * TILES + j) * 2 + l
                gate[l * 72 + j * 8 + r, k] = 1
                gate[144 + l * TILES + j, k] = 1
    head = np.zeros((2, 152, 72), np.float32)
    for r in range(72):
        for l in range(2):
            part, k = r // 36, (r % 36) * 2 + l
            head[part, l * 72 + r, k] = 1
            head[part, 144 + l, k] = 1
    return jnp.asarray(gate, jnp.bfloat16), jnp.asarray(head, jnp.bfloat16)


def serve_kernel(shift, turn, head_turn, same, other, gate_in, qkv_in, sums_in, gate_out, qkv_out, sums, held, held_heads, gate_buf, qkv_buf, in_sems, out_sems):
    del gate_in, qkv_in
    x, y, c = here()
    chip = lax.rem(x + 4 - shift[0], 4) * 4 + lax.rem(y + 4 - shift[1], 4)
    copies = []
    for i, piece in enumerate((same, other)):
        slot = c if i == 0 else 1 - c
        for p in range(2):
            copies.append(
                pltpu.make_async_copy(
                    piece.at[pl.ds(p * GATE_ROWS, GATE_ROWS)],
                    held.at[slot, p, pl.ds(pl.multiple_of(slot * 8, 8), GATE_ROWS)],
                    in_sems.at[i, p],
                )
            )
        copies.append(
            pltpu.make_async_copy(
                piece.at[pl.ds(2 * GATE_ROWS, 2 * HEAD_ROWS)], held_heads.at[slot], in_sems.at[i, 2]
            )
        )
    for copy in copies:
        copy.start()
    for copy in copies:
        copy.wait()

    def both(slot, start, length):
        return jnp.concatenate([held[slot, p, pl.ds(start, length)] for p in range(2)], axis=1)

    def dot(a, b):
        return jnp.dot(a, b, preferred_element_type=jnp.float32)

    gate_sum = jnp.zeros((24, 256), jnp.float32)
    for g in range(9):
        if g < 4:
            got = dot(turn[...], both(0, 144 * g, 144))
        elif g > 4:
            got = dot(turn[...], both(1, 80 + 144 * (g - 5), 144))
        else:
            got = dot(turn[:, :72], both(0, 576, 72)) + dot(turn[:, 72:], both(1, 8, 72))
        for l in range(2):
            for p in range(2):
                gate_buf[l, pl.ds(144 * g + 72 * p, 72), :] = got[l * 72 : (l + 1) * 72, p * 128 : (p + 1) * 128].astype(jnp.bfloat16)
        gate_sum += got[144:168]
    got = None
    for part in range(2):
        heads = jnp.concatenate([held_heads[part, pl.ds(72 * k, 72)] for k in range(2)], axis=1)
        term = dot(head_turn[part], heads)
        got = term if got is None else got + term
    for l in range(2):
        for g in range(9):
            for k in range(2):
                qkv_buf[l, pl.ds(16 * g + 8 * k, 8), :] = got[l * 72 + 8 * g : l * 72 + 8 * g + 8, k * 128 : (k + 1) * 128].astype(jnp.bfloat16)
    head_sum = got[144:152]
    if sums_in is not None:
        gate_sum = gate_sum + sums_in[0:24, :]
        head_sum = head_sum + sums_in[24:32, :]
    sums[0:24, :] = gate_sum
    sums[24:32, :] = head_sum
    out = [
        pltpu.make_async_copy(gate_buf, gate_out.at[:, pl.ds(pl.multiple_of(chip * 1296, 16), 1296)], out_sems.at[0]),
        pltpu.make_async_copy(qkv_buf, qkv_out.at[:, pl.ds(pl.multiple_of(chip * 144, 16), 144)], out_sems.at[1]),
    ]
    for copy in out:
        copy.start()
    for copy in out:
        copy.wait()


def serve(shift, turn, head_turn, same, other, done):
    first = done is None
    any_spec = pl.BlockSpec(memory_space=pl.ANY)
    vmem_spec = pl.BlockSpec(memory_space=pltpu.VMEM)
    kernel = functools.partial(serve_kernel, shift)
    if first:
        kernel = lambda a, b, c, d, *rest: serve_kernel(shift, a, b, c, d, None, None, None, *rest)
    pieces = [same.reshape(1440, 128), other.reshape(1440, 128)]
    pieces = [in_hbm(piece) for piece in pieces]
    return pl.pallas_call(
        kernel,
        out_shape=[
            pltpu.HBM((2, 16 * 1296, 128), jnp.bfloat16),
            pltpu.HBM((2, 16 * 144, 128), jnp.bfloat16),
            pltpu.VMEM((32, 256), jnp.float32),
        ],
        in_specs=[vmem_spec, vmem_spec, any_spec, any_spec] + ([] if first else [any_spec, any_spec, vmem_spec]),
        out_specs=[any_spec, any_spec, vmem_spec],
        scratch_shapes=[
            pltpu.VMEM((2, 2, 656, 128), jnp.bfloat16),
            pltpu.VMEM((2, 144, 128), jnp.bfloat16),
            pltpu.VMEM((2, 1296, 128), jnp.bfloat16),
            pltpu.VMEM((2, 144, 128), jnp.bfloat16),
            pltpu.SemaphoreType.DMA((2, 3)),
            pltpu.SemaphoreType.DMA((2,)),
        ],
        input_output_aliases={} if first else {4: 0, 5: 1},
        compiler_params=pltpu.CompilerParams(vmem_limit_bytes=8 << 20),
        cost_estimate=pl.CostEstimate(flops=2 * 168 * 144 * 256 * 10, bytes_accessed=3 << 20, transcendentals=0),
        name="serve",
    )(turn, head_turn, *pieces, *(() if first else done))


def relayout(qkv_weight, gate_up_weight, head_slot, layer_ids, stored_qkv, stored_gate_up):
    owners = lax.axis_size("dev")
    owner = lax.axis_index("dev")
    layers = qkv_weight.shape[0]
    slots = NHEAD // owners
    blocks = FF // owners // BLK
    gate = gate_up_weight.transpose(1, 0, 2).reshape(ROWS, 2, 2 * FF // 128, 128).transpose(0, 2, 1, 3)
    qkv = qkv_weight.transpose(1, 0, 2).reshape(4, 9, 2, NHEAD, HEAD_DIM).transpose(0, 1, 3, 2, 4)

    moves = MOVES
    gate, qkv = in_hbm(gate), in_vmem(qkv)
    pieces = {}
    at, after = 0, ()
    for count in COUNTS:
        part = tuple(moves[at : at + count])
        made = cut(part, head_slot, gate, qkv, after)
        pieces.update(zip(part, made))
        at, after = at + count, (made[-1],)
    got = {}
    for move in moves[:-1]:
        got[move] = lax.ppermute(pieces[move], "dev", moved_pairs(*move))
    got[(0, 0, 0)] = pieces[(0, 0, 0)]

    turn, head_turn = turns()
    done = None
    for shift in [(0, 0)] + ORDER:
        done = serve(shift, turn, head_turn, got[(*shift, 0)], got[(*shift, 1)], done)
    gate_out, qkv_out, total = done
    served_qkv = qkv_out.reshape(2, 144, 2, 8, 128).transpose(0, 1, 3, 2, 4).reshape(2, 1152, 256)
    served_gate = gate_out.reshape(2, 144, 18, 8, 128).transpose(0, 1, 3, 2, 4).reshape(2, 1152, 2304)

    lane = jnp.sum(total.reshape(32, 2, 128), axis=2)
    for step in (2, 1):
        lane = lane + lax.ppermute(lane, "grp", [(g, g ^ step) for g in range(4)])
    block_sum = lane[:18].reshape(2, 9, 2).transpose(0, 2, 1).reshape(2, 18)
    head_sum = lane[24:26]

    layer_pick = (layer_ids[:, None] == jnp.arange(STORED, dtype=jnp.int32)[None, :]).astype(jnp.float32)
    picked_qkv = jnp.dot(layer_pick, stored_qkv.astype(jnp.float32), precision=lax.Precision.HIGHEST, preferred_element_type=jnp.float32)
    picked_gate = jnp.dot(layer_pick, stored_gate_up.astype(jnp.float32), precision=lax.Precision.HIGHEST, preferred_element_type=jnp.float32)
    own_heads = lax.dynamic_slice_in_dim(head_slot, owner * slots, slots, 0)
    picked_qkv = picked_qkv[:, own_heads]
    picked_gate = picked_gate.reshape(layers, 2, owners, blocks).transpose(0, 2, 1, 3).reshape(layers, owners * 2 * blocks)
    picked_gate = lax.dynamic_slice_in_dim(picked_gate, owner * 2 * blocks, 2 * blocks, 1)
    qkv_mismatch = head_sum - picked_qkv * stored_unit
    gate_up_mismatch = block_sum - picked_gate * stored_unit
    return served_qkv, served_gate, qkv_mismatch, gate_up_mismatch


def solution(mesh):
    placed = (P(None, ("grp", "dev"), None), P(None, ("grp", "dev"), None), P(), P(), P(), P())
    return jax.shard_map(
        relayout,
        mesh=mesh,
        in_specs=placed,
        out_specs=(P(None, "grp", "dev"), P(None, "grp", "dev"), P(None, "dev"), P(None, "dev")),
        check_vma=False,
    )
```

```python
import functools

import jax
import jax.numpy as jnp
import numpy as np
from jax import lax
from jax.experimental import pallas as pl
from jax.experimental.pallas import tpu as pltpu
from jax.sharding import PartitionSpec as P


HEAD_DIM = 128
FF = 36864
NHEAD = 64

stored_unit = 1.0 / 1024.0

RINGS = [
    [(1, 1), (3, 3), (1, 3), (3, 1)],
    [(2, 2)],
    [(1, 0), (3, 0), (0, 1), (0, 3)],
    [(2, 0), (0, 2)],
    [(2, 1), (2, 3), (1, 2), (3, 2)],
]
MOVES = [(dx, dy, dc) for ring in RINGS for dc in (0, 1) for dx, dy in ring] + [(0, 0, 1), (0, 0, 0)]
SERVED = [(0, 0)] + [move[:2] for move in MOVES[:-2] if move[2] == 1]
COUNTS = [4, 6, 6, 8, 8]

ROWS = 36
TILES = FF // 32 // 128
PIECE = (2 * ROWS + 8, TILES, 2, 128)
GATE_ROWS = ROWS * TILES * 2
HEAD_ROWS = ROWS * 2


def place_of(me):
    return me // 8, (me // 2) % 4, me % 2


def moved_pairs(dx, dy, dc):
    pairs = []
    for me in range(32):
        x, y, c = place_of(me)
        pairs.append((me, (((x + dx) % 4) * 4 + (y + dy) % 4) * 2 + (c ^ dc)))
    return pairs


def in_hbm(x):
    return pltpu.with_memory_space_constraint(x, pltpu.HBM)


def here():
    me = lax.axis_index("dev")
    return lax.div(me, 8), lax.rem(lax.div(me, 2), 4), lax.rem(me, 2)


def cut_kernel(shifts, heads, gate, qkv, *rest):
    outs, sems = rest[-1 - len(shifts) : -1], rest[-1]
    x, y, c = here()
    copies = []
    for i, ((dx, dy, dc), out) in enumerate(zip(shifts, outs)):
        owner = (lax.rem(x + dx, 4) * 4 + lax.rem(y + dy, 4)) * 2 + lax.rem(c + dc, 2)
        for p in range(2):
            copies.append(
                pltpu.make_async_copy(
                    gate.at[:, pl.ds(p * 32 * TILES + owner * TILES, TILES)],
                    out.at[pl.ds(p * ROWS, ROWS)],
                    sems.at[i, p],
                )
            )
        for k in range(2):
            copies.append(
                pltpu.make_async_copy(
                    qkv.at[:, :, heads[2 * owner + k]],
                    out.at[pl.ds(2 * ROWS + 4 * k, 4)],
                    sems.at[i, 2 + k],
                )
            )
    for copy in copies:
        copy.start()
    for copy in copies:
        copy.wait()


def cut(shifts, heads, gate, qkv, after):
    size = int(np.prod(PIECE)) * 2 * len(shifts)
    return pl.pallas_call(
        functools.partial(cut_kernel, shifts),
        out_shape=[pltpu.VMEM(PIECE, jnp.bfloat16)] * len(shifts),
        in_specs=[pl.BlockSpec(memory_space=pltpu.SMEM)] + [pl.BlockSpec(memory_space=pl.ANY)] * (2 + len(after)),
        out_specs=[pl.BlockSpec(memory_space=pl.ANY)] * len(shifts),
        scratch_shapes=[pltpu.SemaphoreType.DMA((len(shifts), 4))],
        compiler_params=pltpu.CompilerParams(vmem_limit_bytes=1 << 20),
        cost_estimate=pl.CostEstimate(flops=size, bytes_accessed=2 * size, transcendentals=0),
        name="cut",
    )(heads, gate, qkv, *after)


def turns():
    gate = np.zeros((168, 144), np.float32)
    for r in range(8):
        for j in range(TILES):
            for l in range(2):
                k = (r * TILES + j) * 2 + l
                gate[l * 72 + j * 8 + r, k] = 1
                gate[144 + l * TILES + j, k] = 1
    head = np.zeros((2, 152, 72), np.float32)
    for r in range(72):
        for l in range(2):
            part, k = r // 36, (r % 36) * 2 + l
            head[part, l * 72 + r, k] = 1
            head[part, 144 + l, k] = 1
    return jnp.asarray(gate, jnp.bfloat16), jnp.asarray(head, jnp.bfloat16)


def serve_kernel(shift, turn, head_turn, same, other, gate_in, qkv_in, sums_in, gate_out, qkv_out, sums, held, held_heads, gate_buf, qkv_buf, in_sems, out_sems):
    del gate_in, qkv_in
    x, y, c = here()
    chip = lax.rem(x + 4 - shift[0], 4) * 4 + lax.rem(y + 4 - shift[1], 4)
    copies = []
    for i, piece in enumerate((same, other)):
        slot = c if i == 0 else 1 - c
        for p in range(2):
            copies.append(
                pltpu.make_async_copy(
                    piece.at[pl.ds(p * GATE_ROWS, GATE_ROWS)],
                    held.at[slot, p, pl.ds(pl.multiple_of(slot * 8, 8), GATE_ROWS)],
                    in_sems.at[i, p],
                )
            )
        copies.append(
            pltpu.make_async_copy(
                piece.at[pl.ds(2 * GATE_ROWS, 2 * HEAD_ROWS)], held_heads.at[slot], in_sems.at[i, 2]
            )
        )
    for copy in copies:
        copy.start()
    for copy in copies:
        copy.wait()

    def both(slot, start, length):
        return jnp.concatenate([held[slot, p, pl.ds(start, length)] for p in range(2)], axis=1)

    def dot(a, b):
        return jnp.dot(a, b, preferred_element_type=jnp.float32)

    gate_sum = jnp.zeros((24, 256), jnp.float32)
    copies = []
    for g in range(9):
        if g < 4:
            got = dot(turn[...], both(0, 144 * g, 144))
        elif g > 4:
            got = dot(turn[...], both(1, 80 + 144 * (g - 5), 144))
        else:
            got = dot(turn[:, :72], both(0, 576, 72)) + dot(turn[:, 72:], both(1, 8, 72))
        for l in range(2):
            for p in range(2):
                gate_buf[l, pl.ds(144 * g + 72 * p, 72), :] = got[l * 72 : (l + 1) * 72, p * 128 : (p + 1) * 128].astype(jnp.bfloat16)
        gate_sum += got[144:168]
        copies.append(
            pltpu.make_async_copy(
                gate_buf.at[:, pl.ds(144 * g, 144)],
                gate_out.at[:, pl.ds(pl.multiple_of(chip * 1296 + 144 * g, 16), 144)],
                out_sems.at[g],
            )
        )
        copies[-1].start()
    got = None
    for part in range(2):
        heads = jnp.concatenate([held_heads[part, pl.ds(72 * k, 72)] for k in range(2)], axis=1)
        term = dot(head_turn[part], heads)
        got = term if got is None else got + term
    for l in range(2):
        for g in range(9):
            for k in range(2):
                qkv_buf[l, pl.ds(16 * g + 8 * k, 8), :] = got[l * 72 + 8 * g : l * 72 + 8 * g + 8, k * 128 : (k + 1) * 128].astype(jnp.bfloat16)
    head_sum = got[144:152]
    if sums_in is not None:
        gate_sum = gate_sum + sums_in[0:24, :]
        head_sum = head_sum + sums_in[24:32, :]
    sums[0:24, :] = gate_sum
    sums[24:32, :] = head_sum
    copies.append(
        pltpu.make_async_copy(qkv_buf, qkv_out.at[:, pl.ds(pl.multiple_of(chip * 144, 16), 144)], out_sems.at[9])
    )
    copies[-1].start()
    for copy in copies:
        copy.wait()


def serve(shift, turn, head_turn, same, other, done):
    first = done is None
    any_spec = pl.BlockSpec(memory_space=pl.ANY)
    vmem_spec = pl.BlockSpec(memory_space=pltpu.VMEM)
    kernel = functools.partial(serve_kernel, shift)
    if first:
        kernel = lambda a, b, c, d, *rest: serve_kernel(shift, a, b, c, d, None, None, None, *rest)
    pieces = [same.reshape(1440, 128), other.reshape(1440, 128)]
    return pl.pallas_call(
        kernel,
        out_shape=[
            pltpu.HBM((2, 16 * 1296, 128), jnp.bfloat16),
            pltpu.HBM((2, 16 * 144, 128), jnp.bfloat16),
            pltpu.VMEM((32, 256), jnp.float32),
        ],
        in_specs=[vmem_spec, vmem_spec, any_spec, any_spec] + ([] if first else [any_spec, any_spec, vmem_spec]),
        out_specs=[any_spec, any_spec, vmem_spec],
        scratch_shapes=[
            pltpu.VMEM((2, 2, 656, 128), jnp.bfloat16),
            pltpu.VMEM((2, 144, 128), jnp.bfloat16),
            pltpu.VMEM((2, 1296, 128), jnp.bfloat16),
            pltpu.VMEM((2, 144, 128), jnp.bfloat16),
            pltpu.SemaphoreType.DMA((2, 3)),
            pltpu.SemaphoreType.DMA((10,)),
        ],
        input_output_aliases={} if first else {4: 0, 5: 1},
        compiler_params=pltpu.CompilerParams(vmem_limit_bytes=8 << 20),
        cost_estimate=pl.CostEstimate(flops=2 * 168 * 144 * 256 * 10, bytes_accessed=3 << 20, transcendentals=0),
        name="serve",
    )(turn, head_turn, *pieces, *(() if first else done))


def picks():
    gate = np.zeros((24, GATE_ROWS), np.float32)
    for k in range(GATE_ROWS):
        gate[(k % 2) * TILES + k // 2 % TILES, k] = 1
    head = np.zeros((8, HEAD_ROWS), np.float32)
    for k in range(HEAD_ROWS):
        head[k % 2, k] = 1
    return jnp.asarray(gate, jnp.bfloat16), jnp.asarray(head, jnp.bfloat16)


def tally_kernel(gate, head, before, same, other, out):
    for p in range(2):
        lanes = slice(128 * p, 128 * (p + 1))
        gates, heads = before[0:24, lanes], before[24:32, lanes]
        for piece in (same, other):
            rows = piece[pl.ds(GATE_ROWS * p, GATE_ROWS)]
            gates += jnp.dot(gate[...], rows, preferred_element_type=jnp.float32)
            rows = piece[pl.ds(2 * GATE_ROWS + HEAD_ROWS * p, HEAD_ROWS)]
            heads += jnp.dot(head[...], rows, preferred_element_type=jnp.float32)
        out[0:24, lanes] = gates
        out[24:32, lanes] = heads


def tally(before, pieces):
    vmem_spec = pl.BlockSpec(memory_space=pltpu.VMEM)
    return pl.pallas_call(
        tally_kernel,
        out_shape=pltpu.VMEM((32, 256), jnp.float32),
        in_specs=[vmem_spec] * 5,
        out_specs=vmem_spec,
        compiler_params=pltpu.CompilerParams(vmem_limit_bytes=4 << 20),
        name="tally",
    )(*picks(), before, *[piece.reshape(1440, 128) for piece in pieces])


def pick_kernel(heads, layer_ids, stored_qkv, stored_gate, gate_pick, qkv_pick):
    owner = lax.axis_index("dev")

    def table(width, value):
        row = lax.broadcasted_iota(jnp.int32, (2, width), 0)
        column = lax.broadcasted_iota(jnp.int32, (2, width), 1)
        out = jnp.zeros((2, width), jnp.int32)
        for l in range(2):
            for b in range(width):
                out = jnp.where((row == l) & (column == b), value(layer_ids[l], b), out)
        return out.astype(jnp.float32) * stored_unit

    gate_pick[...] = table(18, lambda l, b: stored_gate[l, (b // TILES) * 32 * TILES + owner * TILES + b % TILES])
    qkv_pick[...] = table(2, lambda l, b: stored_qkv[l, heads[2 * owner + b]])


def pick(heads, layer_ids, stored_qkv, stored_gate):
    return pl.pallas_call(
        pick_kernel,
        out_shape=[pltpu.VMEM((2, 18), jnp.float32), pltpu.VMEM((2, 2), jnp.float32)],
        in_specs=[pl.BlockSpec(memory_space=pltpu.SMEM)] * 4,
        out_specs=[pl.BlockSpec(memory_space=pltpu.VMEM)] * 2,
        compiler_params=pltpu.CompilerParams(vmem_limit_bytes=1 << 20),
        name="pick",
    )(heads, layer_ids, stored_qkv, stored_gate)


def settle_kernel(a, b, c, d, gate_pick, qkv_pick, gate_out, qkv_out):
    total = (a[...] + b[...] + c[...] + d[...]).T
    sums = [jnp.sum(total[128 * p : 128 * (p + 1)], axis=0, keepdims=True) for p in range(2)]
    for l in range(2):
        row = jnp.concatenate([s[:, TILES * l : TILES * (l + 1)] for s in sums], axis=1)
        gate_out[l : l + 1, :] = row - gate_pick[l : l + 1, :]
        row = jnp.concatenate([s[:, 24 + l : 25 + l] for s in sums], axis=1)
        qkv_out[l : l + 1, :] = row - qkv_pick[l : l + 1, :]


def settle(totals, gate_pick, qkv_pick):
    return pl.pallas_call(
        settle_kernel,
        out_shape=[jax.ShapeDtypeStruct((2, 18), jnp.float32), jax.ShapeDtypeStruct((2, 2), jnp.float32)],
        in_specs=[pl.BlockSpec(memory_space=pltpu.VMEM)] * 6,
        out_specs=[pl.BlockSpec(memory_space=pltpu.VMEM)] * 2,
        compiler_params=pltpu.CompilerParams(vmem_limit_bytes=1 << 20),
        name="settle",
    )(*totals, gate_pick, qkv_pick)


def relayout(qkv_weight, gate_up_weight, head_slot, layer_ids, stored_qkv, stored_gate_up):
    gate = gate_up_weight.transpose(1, 0, 2).reshape(ROWS, 2, 2 * FF // 128, 128).transpose(0, 2, 1, 3)
    qkv = qkv_weight.transpose(1, 0, 2).reshape(4, 9, 2, NHEAD, HEAD_DIM).transpose(0, 1, 3, 2, 4)

    moves = MOVES
    gate, qkv = in_hbm(gate), in_hbm(qkv)
    pieces = {}
    at, after = 0, ()
    for count in COUNTS:
        part = tuple(moves[at : at + count])
        made = cut(part, head_slot, gate, qkv, after)
        pieces.update(zip(part, made))
        at, after = at + count, (made[-1],)
    got = {}
    for move in moves[:-1]:
        got[move] = lax.ppermute(pieces[move], "dev", moved_pairs(*move))
    got[(0, 0, 0)] = pieces[(0, 0, 0)]

    turn, head_turn = turns()
    done = None
    for i, shift in enumerate(SERVED):
        if i == len(SERVED) - 1:
            totals = [tally(done[2], [got[(*shift, dc)] for dc in (0, 1)])]
            for step in (1, 2, 3):
                totals.append(lax.ppermute(totals[0], "grp", [(g, (g + step) % 4) for g in range(4)]))
        done = serve(shift, turn, head_turn, got[(*shift, 0)], got[(*shift, 1)], done)
    gate_out, qkv_out = done[:2]
    served_qkv = qkv_out.reshape(2, 144, 2, 8, 128).transpose(0, 1, 3, 2, 4).reshape(2, 1152, 256)
    served_gate = gate_out.reshape(2, 144, 18, 8, 128).transpose(0, 1, 3, 2, 4).reshape(2, 1152, 2304)

    gate_pick, qkv_pick = pick(head_slot, layer_ids, stored_qkv, stored_gate_up)
    gate_up_mismatch, qkv_mismatch = settle(totals, gate_pick, qkv_pick)
    return served_qkv, served_gate, qkv_mismatch, gate_up_mismatch


def solution(mesh):
    placed = (P(None, ("grp", "dev"), None), P(None, ("grp", "dev"), None), P(), P(), P(), P())
    return jax.shard_map(
        relayout,
        mesh=mesh,
        in_specs=placed,
        out_specs=(P(None, "grp", "dev"), P(None, "grp", "dev"), P(None, "dev"), P(None, "dev")),
        check_vma=False,
    )
```

```python
import functools

import jax
import jax.numpy as jnp
import numpy as np
from jax import lax
from jax.experimental import pallas as pl
from jax.experimental.pallas import tpu as pltpu
from jax.sharding import PartitionSpec as P


HEAD_DIM = 128
FF = 36864
NHEAD = 64

stored_unit = 1.0 / 1024.0

RINGS = [
    [(1, 1), (3, 3), (1, 3), (3, 1)],
    [(2, 2)],
    [(1, 0), (3, 0), (0, 1), (0, 3)],
    [(2, 0), (0, 2)],
    [(2, 1), (2, 3), (1, 2), (3, 2)],
]
MOVES = [(dx, dy, dc) for ring in RINGS for dc in (0, 1) for dx, dy in ring] + [(0, 0, 1), (0, 0, 0)]
SERVED = [(0, 0)] + [move[:2] for move in MOVES[:-2] if move[2] == 1]
COUNTS = [4, 6, 6, 8, 8]

ROWS = 36
TILES = FF // 32 // 128
PIECE = (2 * ROWS + 8, TILES, 2, 128)
GATE_ROWS = ROWS * TILES * 2
HEAD_ROWS = ROWS * 2


def place_of(me):
    return me // 8, (me // 2) % 4, me % 2


def moved_pairs(dx, dy, dc):
    pairs = []
    for me in range(32):
        x, y, c = place_of(me)
        pairs.append((me, (((x + dx) % 4) * 4 + (y + dy) % 4) * 2 + (c ^ dc)))
    return pairs


def in_hbm(x):
    return pltpu.with_memory_space_constraint(x, pltpu.HBM)


def here():
    me = lax.axis_index("dev")
    return lax.div(me, 8), lax.rem(lax.div(me, 2), 4), lax.rem(me, 2)


def cut_kernel(shifts, heads, gate, qkv, *rest):
    outs, sems = rest[-1 - len(shifts) : -1], rest[-1]
    x, y, c = here()
    copies = []
    for i, ((dx, dy, dc), out) in enumerate(zip(shifts, outs)):
        owner = (lax.rem(x + dx, 4) * 4 + lax.rem(y + dy, 4)) * 2 + lax.rem(c + dc, 2)
        for p in range(2):
            copies.append(
                pltpu.make_async_copy(
                    gate.at[:, pl.ds(p * 32 * TILES + owner * TILES, TILES)],
                    out.at[pl.ds(p * ROWS, ROWS)],
                    sems.at[i, p],
                )
            )
        for k in range(2):
            copies.append(
                pltpu.make_async_copy(
                    qkv.at[:, :, heads[2 * owner + k]],
                    out.at[pl.ds(2 * ROWS + 4 * k, 4)],
                    sems.at[i, 2 + k],
                )
            )
    for copy in copies:
        copy.start()
    for copy in copies:
        copy.wait()


def cut(shifts, heads, gate, qkv, after):
    size = int(np.prod(PIECE)) * 2 * len(shifts)
    return pl.pallas_call(
        functools.partial(cut_kernel, shifts),
        out_shape=[pltpu.VMEM(PIECE, jnp.bfloat16)] * len(shifts),
        in_specs=[pl.BlockSpec(memory_space=pltpu.SMEM)] + [pl.BlockSpec(memory_space=pl.ANY)] * (2 + len(after)),
        out_specs=[pl.BlockSpec(memory_space=pl.ANY)] * len(shifts),
        scratch_shapes=[pltpu.SemaphoreType.DMA((len(shifts), 4))],
        compiler_params=pltpu.CompilerParams(vmem_limit_bytes=1 << 20),
        cost_estimate=pl.CostEstimate(flops=size, bytes_accessed=2 * size, transcendentals=0),
        name="cut",
    )(heads, gate, qkv, *after)


def turns():
    gate = np.zeros((168, 144), np.float32)
    for r in range(8):
        for j in range(TILES):
            for l in range(2):
                k = (r * TILES + j) * 2 + l
                gate[l * 72 + j * 8 + r, k] = 1
                gate[144 + l * TILES + j, k] = 1
    head = np.zeros((2, 152, 72), np.float32)
    for r in range(72):
        for l in range(2):
            part, k = r // 36, (r % 36) * 2 + l
            head[part, l * 72 + r, k] = 1
            head[part, 144 + l, k] = 1
    return jnp.asarray(gate, jnp.bfloat16), jnp.asarray(head, jnp.bfloat16)


def serve_kernel(shift, turn, head_turn, same, other, gate_in, qkv_in, sums_in, gate_out, qkv_out, sums, held, held_heads, gate_buf, qkv_buf, in_sems, out_sems):
    del gate_in, qkv_in
    x, y, c = here()
    chip = lax.rem(x + 4 - shift[0], 4) * 4 + lax.rem(y + 4 - shift[1], 4)
    copies = []
    for i, piece in enumerate((same, other)):
        slot = c if i == 0 else 1 - c
        for p in range(2):
            copies.append(
                pltpu.make_async_copy(
                    piece.at[pl.ds(p * GATE_ROWS, GATE_ROWS)],
                    held.at[slot, p, pl.ds(pl.multiple_of(slot * 8, 8), GATE_ROWS)],
                    in_sems.at[i, p],
                )
            )
        copies.append(
            pltpu.make_async_copy(
                piece.at[pl.ds(2 * GATE_ROWS, 2 * HEAD_ROWS)], held_heads.at[slot], in_sems.at[i, 2]
            )
        )
    for copy in copies:
        copy.start()
    for copy in copies:
        copy.wait()

    def both(slot, start, length):
        return jnp.concatenate([held[slot, p, pl.ds(start, length)] for p in range(2)], axis=1)

    def dot(a, b):
        return jnp.dot(a, b, preferred_element_type=jnp.float32)

    gate_sum = jnp.zeros((24, 256), jnp.float32)
    copies = []
    for g in range(9):
        if g < 4:
            got = dot(turn[...], both(0, 144 * g, 144))
        elif g > 4:
            got = dot(turn[...], both(1, 80 + 144 * (g - 5), 144))
        else:
            got = dot(turn[:, :72], both(0, 576, 72)) + dot(turn[:, 72:], both(1, 8, 72))
        for l in range(2):
            for p in range(2):
                gate_buf[l, pl.ds(144 * g + 72 * p, 72), :] = got[l * 72 : (l + 1) * 72, p * 128 : (p + 1) * 128].astype(jnp.bfloat16)
        gate_sum += got[144:168]
        copies.append(
            pltpu.make_async_copy(
                gate_buf.at[:, pl.ds(144 * g, 144)],
                gate_out.at[:, pl.ds(pl.multiple_of(chip * 1296 + 144 * g, 16), 144)],
                out_sems.at[g],
            )
        )
        copies[-1].start()
    got = None
    for part in range(2):
        heads = jnp.concatenate([held_heads[part, pl.ds(72 * k, 72)] for k in range(2)], axis=1)
        term = dot(head_turn[part], heads)
        got = term if got is None else got + term
    for l in range(2):
        for g in range(9):
            for k in range(2):
                qkv_buf[l, pl.ds(16 * g + 8 * k, 8), :] = got[l * 72 + 8 * g : l * 72 + 8 * g + 8, k * 128 : (k + 1) * 128].astype(jnp.bfloat16)
    head_sum = got[144:152]
    if sums_in is not None:
        gate_sum = gate_sum + sums_in[0:24, :]
        head_sum = head_sum + sums_in[24:32, :]
    sums[0:24, :] = gate_sum
    sums[24:32, :] = head_sum
    copies.append(
        pltpu.make_async_copy(qkv_buf, qkv_out.at[:, pl.ds(pl.multiple_of(chip * 144, 16), 144)], out_sems.at[9])
    )
    copies[-1].start()
    for copy in copies:
        copy.wait()


def serve(shift, turn, head_turn, same, other, done):
    first = done is None
    any_spec = pl.BlockSpec(memory_space=pl.ANY)
    vmem_spec = pl.BlockSpec(memory_space=pltpu.VMEM)
    kernel = functools.partial(serve_kernel, shift)
    if first:
        kernel = lambda a, b, c, d, *rest: serve_kernel(shift, a, b, c, d, None, None, None, *rest)
    pieces = [same.reshape(1440, 128), other.reshape(1440, 128)]
    return pl.pallas_call(
        kernel,
        out_shape=[
            pltpu.HBM((2, 16 * 1296, 128), jnp.bfloat16),
            pltpu.HBM((2, 16 * 144, 128), jnp.bfloat16),
            pltpu.VMEM((32, 256), jnp.float32),
        ],
        in_specs=[vmem_spec, vmem_spec, any_spec, any_spec] + ([] if first else [any_spec, any_spec, vmem_spec]),
        out_specs=[any_spec, any_spec, vmem_spec],
        scratch_shapes=[
            pltpu.VMEM((2, 2, 656, 128), jnp.bfloat16),
            pltpu.VMEM((2, 144, 128), jnp.bfloat16),
            pltpu.VMEM((2, 1296, 128), jnp.bfloat16),
            pltpu.VMEM((2, 144, 128), jnp.bfloat16),
            pltpu.SemaphoreType.DMA((2, 3)),
            pltpu.SemaphoreType.DMA((10,)),
        ],
        input_output_aliases={} if first else {4: 0, 5: 1},
        compiler_params=pltpu.CompilerParams(vmem_limit_bytes=8 << 20),
        cost_estimate=pl.CostEstimate(flops=2 * 168 * 144 * 256 * 10, bytes_accessed=3 << 20, transcendentals=0),
        name="serve",
    )(turn, head_turn, *pieces, *(() if first else done))


def picks():
    gate = np.zeros((24, GATE_ROWS), np.float32)
    for k in range(GATE_ROWS):
        gate[(k % 2) * TILES + k // 2 % TILES, k] = 1
    head = np.zeros((8, HEAD_ROWS), np.float32)
    for k in range(HEAD_ROWS):
        head[k % 2, k] = 1
    return jnp.asarray(gate, jnp.bfloat16), jnp.asarray(head, jnp.bfloat16)


def tally_kernel(gate, head, before, *refs):
    pieces, out = refs[:-1], refs[-1]
    for p in range(2):
        lanes = slice(128 * p, 128 * (p + 1))
        gates, heads = before[0:24, lanes], before[24:32, lanes]
        for piece in pieces:
            rows = piece[pl.ds(GATE_ROWS * p, GATE_ROWS)]
            gates += jnp.dot(gate[...], rows, preferred_element_type=jnp.float32)
            rows = piece[pl.ds(2 * GATE_ROWS + HEAD_ROWS * p, HEAD_ROWS)]
            heads += jnp.dot(head[...], rows, preferred_element_type=jnp.float32)
        out[0:24, lanes] = gates
        out[24:32, lanes] = heads


def tally(before, pieces):
    vmem_spec = pl.BlockSpec(memory_space=pltpu.VMEM)
    return pl.pallas_call(
        tally_kernel,
        out_shape=pltpu.VMEM((32, 256), jnp.float32),
        in_specs=[vmem_spec] * (3 + len(pieces)),
        out_specs=vmem_spec,
        compiler_params=pltpu.CompilerParams(vmem_limit_bytes=4 << 20),
        name="tally",
    )(*picks(), before, *[piece.reshape(1440, 128) for piece in pieces])


def merge_kernel(a, b, out):
    out[...] = a[...] + b[...]


def merge(a, b):
    vmem_spec = pl.BlockSpec(memory_space=pltpu.VMEM)
    return pl.pallas_call(
        merge_kernel,
        out_shape=pltpu.VMEM((32, 256), jnp.float32),
        in_specs=[vmem_spec] * 2,
        out_specs=vmem_spec,
        compiler_params=pltpu.CompilerParams(vmem_limit_bytes=1 << 20),
        name="merge",
    )(a, b)


def pick_kernel(heads, layer_ids, stored_qkv, stored_gate, gate_pick, qkv_pick):
    owner = lax.axis_index("dev")

    def table(width, value):
        row = lax.broadcasted_iota(jnp.int32, (2, width), 0)
        column = lax.broadcasted_iota(jnp.int32, (2, width), 1)
        out = jnp.zeros((2, width), jnp.int32)
        for l in range(2):
            for b in range(width):
                out = jnp.where((row == l) & (column == b), value(layer_ids[l], b), out)
        return out.astype(jnp.float32) * stored_unit

    gate_pick[...] = table(18, lambda l, b: stored_gate[l, (b // TILES) * 32 * TILES + owner * TILES + b % TILES])
    qkv_pick[...] = table(2, lambda l, b: stored_qkv[l, heads[2 * owner + b]])


def pick(heads, layer_ids, stored_qkv, stored_gate):
    return pl.pallas_call(
        pick_kernel,
        out_shape=[pltpu.VMEM((2, 18), jnp.float32), pltpu.VMEM((2, 2), jnp.float32)],
        in_specs=[pl.BlockSpec(memory_space=pltpu.SMEM)] * 4,
        out_specs=[pl.BlockSpec(memory_space=pltpu.VMEM)] * 2,
        compiler_params=pltpu.CompilerParams(vmem_limit_bytes=1 << 20),
        name="pick",
    )(heads, layer_ids, stored_qkv, stored_gate)


def settle_kernel(a, b, gate_pick, qkv_pick, gate_out, qkv_out):
    total = (a[...] + b[...]).T
    sums = [jnp.sum(total[128 * p : 128 * (p + 1)], axis=0, keepdims=True) for p in range(2)]
    for l in range(2):
        row = jnp.concatenate([s[:, TILES * l : TILES * (l + 1)] for s in sums], axis=1)
        gate_out[l : l + 1, :] = row - gate_pick[l : l + 1, :]
        row = jnp.concatenate([s[:, 24 + l : 25 + l] for s in sums], axis=1)
        qkv_out[l : l + 1, :] = row - qkv_pick[l : l + 1, :]


def settle(totals, gate_pick, qkv_pick):
    return pl.pallas_call(
        settle_kernel,
        out_shape=[jax.ShapeDtypeStruct((2, 18), jnp.float32), jax.ShapeDtypeStruct((2, 2), jnp.float32)],
        in_specs=[pl.BlockSpec(memory_space=pltpu.VMEM)] * 4,
        out_specs=[pl.BlockSpec(memory_space=pltpu.VMEM)] * 2,
        compiler_params=pltpu.CompilerParams(vmem_limit_bytes=1 << 20),
        name="settle",
    )(*totals, gate_pick, qkv_pick)


def relayout(qkv_weight, gate_up_weight, head_slot, layer_ids, stored_qkv, stored_gate_up):
    gate = gate_up_weight.transpose(1, 0, 2).reshape(ROWS, 2, 2 * FF // 128, 128).transpose(0, 2, 1, 3)
    qkv = qkv_weight.transpose(1, 0, 2).reshape(4, 9, 2, NHEAD, HEAD_DIM).transpose(0, 1, 3, 2, 4)

    moves = MOVES
    gate, qkv = in_hbm(gate), in_hbm(qkv)
    pieces = {}
    at, after = 0, ()
    for count in COUNTS:
        part = tuple(moves[at : at + count])
        made = cut(part, head_slot, gate, qkv, after)
        pieces.update(zip(part, made))
        at, after = at + count, (made[-1],)
    got = {}
    for move in moves[:-1]:
        got[move] = lax.ppermute(pieces[move], "dev", moved_pairs(*move))
    got[(0, 0, 0)] = pieces[(0, 0, 0)]

    turn, head_turn = turns()
    done = None
    last = len(SERVED) - 1
    for i, shift in enumerate(SERVED):
        if i == last - 1:
            mine = tally(done[2], [got[(*late, dc)] for late in SERVED[-2:] for dc in (0, 1)])
            near = lax.ppermute(mine, "grp", [(0, 1), (1, 0), (2, 3), (3, 2)])
        if i == last:
            mine = merge(mine, near)
            near = lax.ppermute(mine, "grp", [(0, 3), (3, 0), (1, 2), (2, 1)])
        done = serve(shift, turn, head_turn, got[(*shift, 0)], got[(*shift, 1)], done)
    gate_out, qkv_out = done[:2]
    served_qkv = qkv_out.reshape(2, 144, 2, 8, 128).transpose(0, 1, 3, 2, 4).reshape(2, 1152, 256)
    served_gate = gate_out.reshape(2, 144, 18, 8, 128).transpose(0, 1, 3, 2, 4).reshape(2, 1152, 2304)

    gate_pick, qkv_pick = pick(head_slot, layer_ids, stored_qkv, stored_gate_up)
    gate_up_mismatch, qkv_mismatch = settle((mine, near), gate_pick, qkv_pick)
    return served_qkv, served_gate, qkv_mismatch, gate_up_mismatch


def solution(mesh):
    placed = (P(None, ("grp", "dev"), None), P(None, ("grp", "dev"), None), P(), P(), P(), P())
    return jax.shard_map(
        relayout,
        mesh=mesh,
        in_specs=placed,
        out_specs=(P(None, "grp", "dev"), P(None, "grp", "dev"), P(None, "dev"), P(None, "dev")),
        check_vma=False,
    )
```
